32 devices in a mesh: dp: 8 (over y, x, core), expert: 4 (over z).
Axes of the slice: x: 2, y: 2, z: 4, core: 2. Of those that a mesh axis runs over, the one named last changes fastest.
Arguments:
- hidden_act: bfloat16 [4096, 2048], P('dp', 'expert'), may hold values from -6 to 6
- out_grad: bfloat16 [4096, 7168], P('dp'), may hold values from -0.125 to 0.125
- counts: int32 [8], P('dp'), may hold values from 0 to 512
- expert_master: float32 [7168, 2048], P('dp', 'expert'), may hold values from -0.005 to 0.005
- expert_mom: float32 [7168, 2048], P('dp', 'expert'), may hold values from -0.12 to 0.12
- expert_var: float32 [7168, 2048], P('dp', 'expert'), may hold values from 0.001 to 0.1
- dense_partial: float32 [8, 4, 14336], P('dp', 'expert'), may hold values from -0.8 to 0.8
- dense_master: float32 [14336], replicated, may hold values from 0.5 to 1.5
- dense_mom: float32 [14336], replicated, may hold values from -2 to 2
- dense_var: float32 [14336], replicated, may hold values from 0.1 to 10
Outputs:
- routed_weight: bfloat16 [7168, 2048], P(None, 'expert')
- new_expert_master: float32 [7168, 2048], P('dp', 'expert')
- new_expert_mom: float32 [7168, 2048], P('dp', 'expert')
- new_expert_var: float32 [7168, 2048], P('dp', 'expert')
- new_dense_master: float32 [14336], replicated
- new_dense_mom: float32 [14336], replicated
- new_dense_var: float32 [14336], replicated
The draws below stay inside these ranges and needn't reach their ends.
All inputs are finite; a program needn't handle non-finite values.
Results may differ from the reference program's by a relative error of at most 0.0004.
Values may be sent and summed in bfloat16 or wider, within the bound.
A program may use at most 128 MiB of HBM per device.

```python
import math
import jax
import jax.numpy as jnp
from jax import lax

D = 7168
FFE = 2048
CAP = 512
ROWS = 4096
GAINS = 14336
N_DP = 8
N_EXPERT = 4


def plant(drawn, key, least, top_value):
    shape = drawn.shape
    index_at = [jax.random.randint(jax.random.fold_in(key, axis), (), 0, shape[axis]) for axis in range(len(shape))]
    drawn = drawn.at[tuple(index_at)].set(least)
    longest = shape.index(max(shape))
    index_at[longest] = (index_at[longest] + 1) % shape[longest]
    return drawn.at[tuple(index_at)].set(top_value)


def with_spikes(result, key, source, target, blocks, factor):
    def block_of(position):
        return (jnp.arange(result.shape[position]) // (result.shape[position] // blocks)).reshape((-1,) + (1,) * (result.ndim - 1 - position))

    one_side = jax.random.permutation(key, blocks)[block_of(target)]
    other_side = (block_of(target) + blocks // 2) % blocks
    return jnp.where((block_of(source) == one_side) | (block_of(source) == other_side), factor * result, result)


def shard_levels(stream_key, dims, cuts, low, top_value):
    def one(position, parts):
        draws = jax.random.uniform(jax.random.fold_in(jax.random.fold_in(stream_key, 6), position), (parts,), jnp.float32, low / len(cuts), top_value / len(cuts))
        return jnp.repeat(jnp.exp(draws), dims[position] // parts).reshape((-1,) + (1,) * (len(dims) - position - 1))

    loudness = one(*cuts[0])
    for cut in cuts[1:]:
        loudness = loudness * one(*cut)
    return loudness


def scatter_about(stream_key, shape, deviation, reach, split=(), kind=jnp.bfloat16):
    gain = shard_levels(stream_key, shape, split, -0.22, 0.18) if split else 1.0
    drawn = jax.random.normal(stream_key, shape, jnp.float32) * deviation * gain
    return jnp.minimum(jnp.maximum(drawn, -reach), reach).astype(kind)


def heavy_noise(own_key, shape, scale, limit, pieces, heavy, held_as=jnp.bfloat16):
    result = scale * jax.random.normal(own_key, shape, jnp.float32)
    if pieces:
        result = result * shard_levels(own_key, shape, pieces, -0.22, 0.18)
    return jnp.clip(with_spikes(result, jax.random.fold_in(own_key, 3), *heavy), -limit, limit).astype(held_as)


def setup_inputs(seed: int = 0) -> dict:
    keys = jax.random.split(jax.random.key(seed), 11)
    hidden_act = scatter_about(keys[0], (ROWS, FFE), 1.0, 6.0, ((0, 8), (1, 4)))
    out_grad = heavy_noise(keys[1], (ROWS, D), ROWS ** -0.5, 0.125, ((0, 8),), (0, 1, 8, 2.0))
    counts = plant(jax.random.randint(keys[2], (N_DP,), 0, CAP + 1), jax.random.fold_in(keys[2], 1), 0, CAP).astype(jnp.int32)
    expert_master = scatter_about(keys[3], (D, FFE), 0.0008, 0.005, ((0, 8), (1, 4)), jnp.float32)
    expert_mom = scatter_about(keys[4], (D, FFE), 0.02, 0.12, ((0, 8), (1, 4)), jnp.float32)
    expert_var = jnp.clip(jnp.exp(math.log(0.1) - 4.6051702 * jax.random.uniform(keys[5], (D, FFE), jnp.float32) ** shard_levels(keys[5], (D, FFE), ((0, 8), (1, 4)), -0.2, 0.2)), 0.001, 0.1)
    dense_partial = heavy_noise(keys[6], (N_DP, N_EXPERT, GAINS), 0.1, 0.8, ((0, 8), (1, 4)), (0, 2, 8, 2.0), jnp.float32)
    dense_master = jnp.clip(1.0 + 0.1 * jax.random.normal(keys[7], (GAINS,), jnp.float32), 0.5, 1.5)
    dense_mom = scatter_about(keys[8], (GAINS,), 0.3, 2.0, (), jnp.float32)
    dense_var = jnp.clip(jnp.exp(jax.random.uniform(keys[9], (GAINS,), jnp.float32, math.log(0.1), math.log(10.0))), 0.1, 10.0)
    return {"hidden_act": hidden_act, "out_grad": out_grad, "counts": counts, "expert_master": expert_master, "expert_mom": expert_mom, "expert_var": expert_var, "dense_partial": dense_partial, "dense_master": dense_master, "dense_mom": dense_mom, "dense_var": dense_var}


beta_one = 0.9
beta_two = 0.95
learn_rate = 0.00022
decay_rate = 0.1
epsilon = 1e-08
step_count = 100

def adamw(gradient, master, moment, second):
    moment_new = beta_one * moment + (1.0 - beta_one) * gradient
    second_new = beta_two * second + (1.0 - beta_two) * gradient * gradient
    first_fix = 1.0 - beta_one ** step_count
    second_fix = 1.0 - beta_two ** step_count
    update = moment_new / first_fix / (jnp.sqrt(second_new / second_fix) + epsilon) + decay_rate * master
    return (master - learn_rate * update, moment_new, second_new)

def reference(hidden_act, out_grad, counts, expert_master, expert_mom, expert_var, dense_partial, dense_master, dense_mom, dense_var):
    row_index = jnp.arange(ROWS, dtype=jnp.int32)
    owners = row_index // CAP
    row_live = row_index % CAP < counts[owners]
    masked = jnp.where(row_live[:, None], hidden_act, jnp.zeros_like(hidden_act))
    expert_grad = jnp.dot(out_grad.T, masked, preferred_element_type=jnp.float32)
    dense_grad = lax.optimization_barrier(jnp.sum(dense_partial, axis=(0, 1)))
    master_new, moment_new, second_new = adamw(expert_grad, expert_master, expert_mom, expert_var)
    dense_new, dense_moment, dense_second = adamw(dense_grad, dense_master, dense_mom, dense_var)
    routed_weight = master_new.astype(jnp.bfloat16)
    return (routed_weight, master_new, moment_new, second_new, dense_new, dense_moment, dense_second)
```

```python
import functools

import jax
import jax.numpy as jnp
from jax import lax
from jax.experimental import pallas as pl
from jax.experimental.pallas import tpu as pltpu
from jax.sharding import PartitionSpec as P

beta_one = 0.9
beta_two = 0.95
learn_rate = 0.00022
decay_rate = 0.1
epsilon = 1e-08
step_count = 100


def adamw(gradient, master, moment, second):
    moment_new = beta_one * moment + (1.0 - beta_one) * gradient
    second_new = beta_two * second + (1.0 - beta_two) * gradient * gradient
    first_fix = 1.0 - beta_one**step_count
    second_fix = 1.0 - beta_two**step_count
    update = (
        moment_new / first_fix / (jnp.sqrt(second_new / second_fix) + epsilon) + decay_rate * master
    )
    return (master - learn_rate * update, moment_new, second_new)


def on_device(
    hidden_act,
    out_grad,
    counts,
    expert_master,
    expert_mom,
    expert_var,
    dense_partial,
    dense_master,
    dense_mom,
    dense_var,
):
    slots = hidden_act.shape[0]
    row_live = lax.iota(jnp.int32, slots) < counts[0]
    masked = jnp.where(row_live[:, None], hidden_act, jnp.zeros_like(hidden_act))
    dense_local = dense_partial.reshape(-1)
    expert_grad = lax.psum_scatter(
        lax.dot_general(
            out_grad, masked, (((0,), (0,)), ((), ())), preferred_element_type=jnp.float32
        ),
        "dp",
        scatter_dimension=0,
        tiled=True,
    )
    dense_grad = lax.psum(dense_local, ("dp", "expert"))
    dense_new, dense_moment, dense_second = adamw(dense_grad, dense_master, dense_mom, dense_var)
    master_new, moment_new, second_new = adamw(expert_grad, expert_master, expert_mom, expert_var)
    routed_weight = lax.all_gather(master_new.astype(jnp.bfloat16), "dp", axis=0, tiled=True)
    return (
        routed_weight,
        master_new,
        moment_new,
        second_new,
        dense_new,
        dense_moment,
        dense_second,
    )


MESH = pl.DeviceIdType.MESH
LANES = 128
DIAG, XN, YN, OWN = 0, 1, 2, 3
TOP = 32767.0


def adamw_kernel(gradient, master, moment, second):
    moment_new = beta_one * moment + (1.0 - beta_one) * gradient
    second_new = beta_two * second + (1.0 - beta_two) * gradient * gradient
    first_fix = 1.0 / (1.0 - beta_one**step_count)
    second_fix = 1.0 / (1.0 - beta_two**step_count)
    update = (
        moment_new * first_fix / (jnp.sqrt(second_new * second_fix) + epsilon) + decay_rate * master
    )
    return (master - learn_rate * update, moment_new, second_new)


def fused_kernel(
    n_z,
    counts_ref,
    hid_ref,
    og_ref,
    p_ref,
    m_ref,
    v_ref,
    dpart_ref,
    dp_ref,
    dm_ref,
    dv_ref,
    w_out,
    p_out,
    m_out,
    v_out,
    dp_out,
    dm_out,
    dv_out,
    hid_raw,
    hid_own,
    hid_peer,
    og_own,
    og_peer,
    part,
    q_send,
    q_recv,
    p_s,
    m_s,
    v_s,
    w_all,
    d_one,
    d_two,
    d_three,
    d_four,
    d_z,
    d_tot,
    load_sem,
    store_sem,
    in_send,
    in_recv,
    rs_send,
    rs_recv,
    ag_send,
    ag_recv,
    peer_send,
    peer_recv,
    place_sem,
    d_send,
    d_recv,
):
    me = lax.axis_index("dp")
    z = lax.axis_index("expert")
    core = lax.rem(me, 2)
    x_at = lax.rem(lax.div(me, 2), 2)
    y_at = lax.div(me, 4)
    flip = 1 - 2 * core
    peer = me + flip
    x_next = me + 2 - 4 * x_at
    y_next = me + 4 - 8 * y_at
    diag = x_next + 4 - 8 * y_at
    owners = (diag, x_next, y_next, me)
    block = p_ref.shape[0]
    width = p_ref.shape[1]
    chunks = width // LANES
    half = d_one.shape[0]

    def og_cols(device):
        return og_ref.at[:, pl.ds(pl.multiple_of(device * block, LANES), block)]

    def cols(k):
        return pl.ds(k * LANES, LANES)

    loads = [pltpu.make_async_copy(hid_ref, hid_raw, load_sem.at[0])]
    for s in range(4):
        loads.append(pltpu.make_async_copy(og_cols(owners[s]), og_own.at[s], load_sem.at[1 + s]))
    for i, (a, b) in enumerate(((p_ref, p_s), (m_ref, m_s), (v_ref, v_s))):
        loads.append(pltpu.make_async_copy(a, b, load_sem.at[5 + i]))
    for copy in loads:
        copy.start()

    barrier = pltpu.get_barrier_semaphore()
    for device in (peer, x_next, y_next):
        pl.semaphore_signal(barrier, inc=1, device_id={"dp": device}, device_id_type=MESH)
    for j in range(1, n_z):
        pl.semaphore_signal(
            barrier, inc=1, device_id={"expert": lax.rem(z + j, n_z)}, device_id_type=MESH
        )
    pl.semaphore_wait(barrier, 3 + n_z - 1)

    def to(device, src, dst, send, recv):
        copy = pltpu.make_async_remote_copy(
            src_ref=src,
            dst_ref=dst,
            send_sem=send,
            recv_sem=recv,
            device_id={"dp": device},
            device_id_type=MESH,
        )
        copy.start()
        return copy

    sends = []
    inputs = {}

    def send_input(s):
        inputs[s] = to(
            peer, og_cols(owners[s] + flip), og_peer.at[s], in_send.at[s], in_recv.at[s]
        )

    send_input(DIAG)
    loads[0].wait()
    live = lax.broadcasted_iota(jnp.int32, hid_raw.shape, 0) < counts_ref[0]
    hid_own[...] = jnp.where(live, hid_raw[...].astype(jnp.float32), 0.0).astype(jnp.bfloat16)
    hid_copy = to(peer, hid_own, hid_peer, in_send.at[4], in_recv.at[4])
    dense_a = to(
        peer,
        dpart_ref.at[pl.ds(pl.multiple_of((1 - core) * half, 8), half)],
        d_one,
        d_send.at[0],
        d_recv.at[0],
    )
    for s in (XN, YN, OWN):
        send_input(s)

    def compute(s):
        loads[1 + s].wait()
        if s == DIAG:
            hid_copy.wait_recv()
        inputs[s].wait_recv()

        @pl.loop(0, block // LANES)
        def _(t):
            at = pl.ds(pl.multiple_of(t * LANES, LANES), LANES)
            dims = (((0,), (0,)), ((), ()))
            part[s, at, :] = lax.dot_general(
                og_own[s, :, at], hid_own[...], dims, preferred_element_type=jnp.float32
            ) + lax.dot_general(
                og_peer[s, :, at], hid_peer[...], dims, preferred_element_type=jnp.float32
            )

    def decoded(i):
        scale = jnp.exp2(q_recv[i, pl.ds(block, 16), :].astype(jnp.int32)[0:1].astype(jnp.float32) * (1.0 / 256.0))
        return q_recv[i, pl.ds(0, block), :].astype(jnp.int32).astype(jnp.float32) * scale

    rs = {}

    def send_sum(device, s, k, value=None):
        i = s * chunks + k
        if value is None:
            value = part[s, :, cols(k)]
        top = jnp.max(jnp.abs(value), axis=0, keepdims=True)
        level = jnp.ceil(jnp.log2(jnp.maximum(top, 1e-30) * (1.0 / TOP)) * 256.0) + 1.0
        q = jnp.round(value * jnp.exp2(level * (-1.0 / 256.0)))
        q_send[i, pl.ds(0, block), :] = q.astype(jnp.int32).astype(jnp.int16)
        q_send[i, pl.ds(block, 16), :] = (
            jnp.broadcast_to(level, (16, LANES)).astype(jnp.int32).astype(jnp.int16)
        )
        rs[s, k] = to(device, q_send.at[i], q_recv.at[i], rs_send.at[i], rs_recv.at[i])

    def first_hop(s, k):
        send_sum((x_next, y_next)[k % 2] if s == DIAG else owners[s], s, k)

    def second_hop(s, k):
        rs[DIAG, k].wait_recv()
        send_sum(owners[s], s, k, part[s, :, cols(k)] + decoded(DIAG * chunks + k))

    compute(DIAG)
    first_hop(DIAG, 0)
    first_hop(DIAG, 1)
    dense_a.wait_recv()
    d_two[0] = dpart_ref[pl.ds(pl.multiple_of(core * half, 8), half), :] + d_one[...]
    dense_b = to(x_next, d_two.at[0], d_two.at[1], d_send.at[1], d_recv.at[1])
    compute(XN)
    first_hop(XN, 0)
    compute(YN)
    first_hop(YN, 1)
    for k in range(2, chunks):
        first_hop(DIAG, k)
    dense_b.wait_recv()
    d_three[0] = d_two[0] + d_two[1]
    dense_c = to(y_next, d_three.at[0], d_three.at[1], d_send.at[2], d_recv.at[2])
    second_hop(XN, 1)
    second_hop(YN, 0)
    compute(OWN)
    dense_c.wait_recv()
    d_four[...] = d_three[0] + d_three[1]
    dense_d = []
    for j in range(1, n_z):
        target = lax.rem(z + j, n_z)
        source = lax.rem(z + n_z - j, n_z)
        copy = pltpu.make_async_remote_copy(
            src_ref=d_four,
            dst_ref=d_z.at[j],
            send_sem=d_send.at[3 + j],
            recv_sem=d_recv.at[3 + j],
            device_id={"expert": target},
            device_id_type=MESH,
        )
        copy.start()
        dense_d.append(copy)
    for k in range(2, chunks):
        first_hop((XN, YN)[k % 2], k)
    for k in range(2, chunks):
        second_hop((YN, XN)[k % 2], k)

    ag = {}
    stores = []
    peers = []
    for i in (5, 6, 7):
        loads[i].wait()

    def spread(s, k):
        rows = pl.ds(pl.multiple_of(owners[s] * block, LANES), block)
        i = s * chunks + k
        src, dst = w_all.at[s, k], w_out.at[rows, cols(k)]
        peers.append(to(peer, src, dst, peer_send.at[i], peer_recv.at[i]))
        copy = pltpu.make_async_copy(src, dst, place_sem.at[i])
        copy.start()
        stores.append(copy)

    def finish(k):
        rs[XN, k].wait_recv()
        rs[YN, k].wait_recv()
        gradient = part[OWN, :, cols(k)] + decoded(XN * chunks + k) + decoded(YN * chunks + k)
        master, moment, second = adamw_kernel(
            gradient, p_s[:, cols(k)], m_s[:, cols(k)], v_s[:, cols(k)]
        )
        w_all[OWN, k] = master.astype(jnp.bfloat16)
        for s, device in ((XN, x_next), (YN, y_next)):
            ag[s, k] = to(
                device,
                w_all.at[OWN, k],
                w_all.at[s, k],
                ag_send.at[s * chunks + k],
                ag_recv.at[s * chunks + k],
            )
        p_s[:, cols(k)] = master
        m_s[:, cols(k)] = moment
        v_s[:, cols(k)] = second
        spread(OWN, k)
        for i, (a, b) in enumerate(((p_s, p_out), (m_s, m_out), (v_s, v_out))):
            copy = pltpu.make_async_copy(
                a.at[:, cols(k)], b.at[:, cols(k)], store_sem.at[i * chunks + k]
            )
            copy.start()
            stores.append(copy)

    for k in range(chunks):
        finish(k)

    for copy in dense_d:
        copy.wait_recv()
    d_z[0] = d_four[...]
    total = None
    for zz in range(n_z):
        term = d_z[lax.rem(z - zz + n_z, n_z)]
        total = term if total is None else total + term
    d_at = pl.ds(pl.multiple_of(core * half, 8), half)
    d_tot[d_at, :] = total
    dense_e = to(peer, d_tot.at[d_at], d_tot.at[d_at], d_send.at[3], d_recv.at[3])

    for k in range(chunks):
        s, device = ((XN, y_next), (YN, x_next))[k % 2]
        ag[s, k].wait_recv()
        ag[DIAG, k] = to(
            device,
            w_all.at[s, k],
            w_all.at[DIAG, k],
            ag_send.at[DIAG * chunks + k],
            ag_recv.at[DIAG * chunks + k],
        )
        spread(s, k)
        other = XN + YN - s
        ag[other, k].wait_recv()
        spread(other, k)

    dense_e.wait_recv()
    d_new = adamw_kernel(d_tot[...], dp_ref[...], dm_ref[...], dv_ref[...])
    dp_out[...], dm_out[...], dv_out[...] = d_new

    for k in range(chunks):
        ag[DIAG, k].wait_recv()
        spread(DIAG, k)

    for copy in list(inputs.values()) + [hid_copy, dense_a, dense_b, dense_c, dense_e] + dense_d:
        copy.wait_send()
    for copy in list(rs.values()) + list(ag.values()):
        copy.wait_send()
    for copy in peers:
        copy.wait()
    for copy in stores:
        copy.wait()


def fused_on_device(
    n_z,
    hidden_act,
    out_grad,
    counts,
    expert_master,
    expert_mom,
    expert_var,
    dense_partial,
    dense_master,
    dense_mom,
    dense_var,
):
    slots, width = hidden_act.shape
    block = expert_master.shape[0]
    chunks = width // LANES
    gains = dense_master.shape[0]
    rows = gains // LANES
    half = rows // 2
    f32, bf16, i16 = jnp.float32, jnp.bfloat16, jnp.int16
    dma = pltpu.SemaphoreType.DMA
    vmem = pl.BlockSpec(memory_space=pltpu.VMEM)
    hbm = pl.BlockSpec(memory_space=pl.ANY)
    outs = pl.pallas_call(
        functools.partial(fused_kernel, n_z),
        out_shape=[
            jax.ShapeDtypeStruct((out_grad.shape[1], width), bf16),
            *[jax.ShapeDtypeStruct((block, width), f32)] * 3,
            *[jax.ShapeDtypeStruct((rows, LANES), f32)] * 3,
        ],
        in_specs=[pl.BlockSpec(memory_space=pltpu.SMEM)] + [hbm] * 5 + [vmem] * 4,
        out_specs=[hbm] * 4 + [vmem] * 3,
        scratch_shapes=[
            pltpu.VMEM((slots, width), bf16),
            pltpu.VMEM((slots, width), bf16),
            pltpu.VMEM((slots, width), bf16),
            pltpu.VMEM((4, slots, block), bf16),
            pltpu.VMEM((4, slots, block), bf16),
            pltpu.VMEM((4, block, width), f32),
            pltpu.VMEM((3 * chunks, block + 16, LANES), i16),
            pltpu.VMEM((3 * chunks, block + 16, LANES), i16),
            pltpu.VMEM((block, width), f32),
            pltpu.VMEM((block, width), f32),
            pltpu.VMEM((block, width), f32),
            pltpu.VMEM((4, chunks, block, LANES), bf16),
            pltpu.VMEM((half, LANES), f32),
            pltpu.VMEM((2, half, LANES), f32),
            pltpu.VMEM((2, half, LANES), f32),
            pltpu.VMEM((half, LANES), f32),
            pltpu.VMEM((n_z, half, LANES), f32),
            pltpu.VMEM((rows, LANES), f32),
            dma((8,)),
            dma((3 * chunks,)),
            dma((5,)),
            dma((5,)),
            dma((3 * chunks,)),
            dma((3 * chunks,)),
            dma((3 * chunks,)),
            dma((3 * chunks,)),
            dma((4 * chunks,)),
            dma((4 * chunks,)),
            dma((4 * chunks,)),
            dma((3 + n_z,)),
            dma((3 + n_z,)),
        ],
        compiler_params=pltpu.CompilerParams(
            collective_id=0, has_side_effects=True, vmem_limit_bytes=56 * 2**20
        ),
    )(
        counts,
        hidden_act,
        out_grad,
        expert_master,
        expert_mom,
        expert_var,
        dense_partial.reshape(rows, LANES),
        dense_master.reshape(rows, LANES),
        dense_mom.reshape(rows, LANES),
        dense_var.reshape(rows, LANES),
    )
    return tuple(outs[:4]) + tuple(a.reshape(gains) for a in outs[4:])


def solution(mesh):
    in_specs = (
        P("dp", "expert"),
        P("dp", None),
        P("dp"),
        P("dp", "expert"),
        P("dp", "expert"),
        P("dp", "expert"),
        P("dp", "expert", None),
        P(),
        P(),
        P(),
    )
    out_specs = (
        P(None, "expert"),
        P("dp", "expert"),
        P("dp", "expert"),
        P("dp", "expert"),
        P(),
        P(),
        P(),
    )
    body = on_device
    if mesh.shape["dp"] == 8:
        body = functools.partial(fused_on_device, mesh.shape["expert"])
    return jax.shard_map(
        body, mesh=mesh, in_specs=in_specs, out_specs=out_specs, check_vma=False
    )
```

```python
import functools

import jax
import jax.numpy as jnp
from jax import lax
from jax.experimental import pallas as pl
from jax.experimental.pallas import tpu as pltpu
from jax.sharding import PartitionSpec as P

beta_one = 0.9
beta_two = 0.95
learn_rate = 0.00022
decay_rate = 0.1
epsilon = 1e-08
step_count = 100


def adamw(gradient, master, moment, second):
    moment_new = beta_one * moment + (1.0 - beta_one) * gradient
    second_new = beta_two * second + (1.0 - beta_two) * gradient * gradient
    first_fix = 1.0 - beta_one**step_count
    second_fix = 1.0 - beta_two**step_count
    update = (
        moment_new / first_fix / (jnp.sqrt(second_new / second_fix) + epsilon) + decay_rate * master
    )
    return (master - learn_rate * update, moment_new, second_new)


def on_device(
    hidden_act,
    out_grad,
    counts,
    expert_master,
    expert_mom,
    expert_var,
    dense_partial,
    dense_master,
    dense_mom,
    dense_var,
):
    slots = hidden_act.shape[0]
    row_live = lax.iota(jnp.int32, slots) < counts[0]
    masked = jnp.where(row_live[:, None], hidden_act, jnp.zeros_like(hidden_act))
    dense_local = dense_partial.reshape(-1)
    expert_grad = lax.psum_scatter(
        lax.dot_general(
            out_grad, masked, (((0,), (0,)), ((), ())), preferred_element_type=jnp.float32
        ),
        "dp",
        scatter_dimension=0,
        tiled=True,
    )
    dense_grad = lax.psum(dense_local, ("dp", "expert"))
    dense_new, dense_moment, dense_second = adamw(dense_grad, dense_master, dense_mom, dense_var)
    master_new, moment_new, second_new = adamw(expert_grad, expert_master, expert_mom, expert_var)
    routed_weight = lax.all_gather(master_new.astype(jnp.bfloat16), "dp", axis=0, tiled=True)
    return (
        routed_weight,
        master_new,
        moment_new,
        second_new,
        dense_new,
        dense_moment,
        dense_second,
    )


MESH = pl.DeviceIdType.MESH
LANES = 128
DIAG, XN, YN, OWN = 0, 1, 2, 3
TOP = 32767.0


def adamw_kernel(gradient, master, moment, second):
    moment_new = beta_one * moment + (1.0 - beta_one) * gradient
    second_new = beta_two * second + (1.0 - beta_two) * gradient * gradient
    first_fix = 1.0 / (1.0 - beta_one**step_count)
    second_fix = 1.0 / (1.0 - beta_two**step_count)
    update = (
        moment_new * first_fix / (jnp.sqrt(second_new * second_fix) + epsilon) + decay_rate * master
    )
    return (master - learn_rate * update, moment_new, second_new)


def fused_kernel(
    n_z,
    counts_ref,
    hid_ref,
    og_ref,
    p_ref,
    m_ref,
    v_ref,
    dpart_ref,
    dp_ref,
    dm_ref,
    dv_ref,
    w_out,
    p_out,
    m_out,
    v_out,
    dp_out,
    dm_out,
    dv_out,
    hid_raw,
    hid_own,
    hid_peer,
    og_own,
    og_peer,
    part,
    q_send,
    q_recv,
    d_one,
    d_two,
    d_three,
    d_four,
    d_z,
    d_tot,
    load_sem,
    in_send,
    in_recv,
    rs_send,
    rs_recv,
    ag_send,
    ag_recv,
    peer_send,
    peer_recv,
    d_send,
    d_recv,
):
    me = lax.axis_index("dp")
    z = lax.axis_index("expert")
    core = lax.rem(me, 2)
    x_at = lax.rem(lax.div(me, 2), 2)
    y_at = lax.div(me, 4)
    flip = 1 - 2 * core
    peer = me + flip
    x_next = me + 2 - 4 * x_at
    y_next = me + 4 - 8 * y_at
    diag = x_next + 4 - 8 * y_at
    owners = (diag, x_next, y_next, me)
    block = p_ref.shape[0]
    width = p_ref.shape[1]
    chunks = width // LANES
    half = d_one.shape[0]

    def og_cols(device):
        return og_ref.at[:, pl.ds(pl.multiple_of(device * block, LANES), block)]

    def cols(k):
        return pl.ds(k * LANES, LANES)

    loads = [pltpu.make_async_copy(hid_ref, hid_raw, load_sem.at[0])]
    for s in range(4):
        loads.append(pltpu.make_async_copy(og_cols(owners[s]), og_own.at[s], load_sem.at[1 + s]))
    for i, (a, b) in enumerate(((p_ref, p_out), (m_ref, m_out), (v_ref, v_out))):
        loads.append(pltpu.make_async_copy(a, b, load_sem.at[5 + i]))
    for copy in loads:
        copy.start()

    barrier = pltpu.get_barrier_semaphore()
    for device in (peer, x_next, y_next):
        pl.semaphore_signal(barrier, inc=1, device_id={"dp": device}, device_id_type=MESH)
    for j in range(1, n_z):
        pl.semaphore_signal(
            barrier, inc=1, device_id={"expert": lax.rem(z + j, n_z)}, device_id_type=MESH
        )
    pl.semaphore_wait(barrier, 3 + n_z - 1)

    def to(device, src, dst, send, recv):
        copy = pltpu.make_async_remote_copy(
            src_ref=src,
            dst_ref=dst,
            send_sem=send,
            recv_sem=recv,
            device_id={"dp": device},
            device_id_type=MESH,
        )
        copy.start()
        return copy

    sends = []
    inputs = {}

    def send_input(s):
        inputs[s] = to(
            peer, og_cols(owners[s] + flip), og_peer.at[s], in_send.at[s], in_recv.at[s]
        )

    send_input(DIAG)
    loads[0].wait()
    live = lax.broadcasted_iota(jnp.int32, hid_raw.shape, 0) < counts_ref[0]
    hid_own[...] = jnp.where(live, hid_raw[...].astype(jnp.float32), 0.0).astype(jnp.bfloat16)
    hid_copy = to(peer, hid_own, hid_peer, in_send.at[4], in_recv.at[4])
    dense_a = to(
        peer,
        dpart_ref.at[pl.ds(pl.multiple_of((1 - core) * half, 8), half)],
        d_one,
        d_send.at[0],
        d_recv.at[0],
    )
    for s in (XN, YN, OWN):
        send_input(s)

    def compute(s):
        loads[1 + s].wait()
        if s == DIAG:
            hid_copy.wait_recv()
        inputs[s].wait_recv()

        @pl.loop(0, block // LANES)
        def _(t):
            at = pl.ds(pl.multiple_of(t * LANES, LANES), LANES)
            dims = (((0,), (0,)), ((), ()))
            part[s, at, :] = lax.dot_general(
                og_own[s, :, at], hid_own[...], dims, preferred_element_type=jnp.float32
            ) + lax.dot_general(
                og_peer[s, :, at], hid_peer[...], dims, preferred_element_type=jnp.float32
            )

    def decoded(i):
        scale = jnp.exp2(q_recv[i, pl.ds(block, 16), :].astype(jnp.int32)[0:1].astype(jnp.float32) * (1.0 / 256.0))
        return q_recv[i, pl.ds(0, block), :].astype(jnp.int32).astype(jnp.float32) * scale

    rs = {}

    def send_sum(device, s, k, value=None):
        i = s * chunks + k
        if value is None:
            value = part[s, :, cols(k)]
        top = jnp.max(jnp.abs(value), axis=0, keepdims=True)
        level = jnp.ceil(jnp.log2(jnp.maximum(top, 1e-30) * (1.0 / TOP)) * 256.0) + 1.0
        q = jnp.round(value * jnp.exp2(level * (-1.0 / 256.0)))
        q_send[i, pl.ds(0, block), :] = q.astype(jnp.int32).astype(jnp.int16)
        q_send[i, pl.ds(block, 16), :] = (
            jnp.broadcast_to(level, (16, LANES)).astype(jnp.int32).astype(jnp.int16)
        )
        rs[s, k] = to(device, q_send.at[i], q_recv.at[i], rs_send.at[i], rs_recv.at[i])

    def first_hop(s, k):
        send_sum((x_next, y_next)[k % 2] if s == DIAG else owners[s], s, k)

    def second_hop(s, k):
        rs[DIAG, k].wait_recv()
        send_sum(owners[s], s, k, part[s, :, cols(k)] + decoded(DIAG * chunks + k))

    compute(DIAG)
    first_hop(DIAG, 0)
    first_hop(DIAG, 1)
    dense_a.wait_recv()
    d_two[0] = dpart_ref[pl.ds(pl.multiple_of(core * half, 8), half), :] + d_one[...]
    dense_b = to(x_next, d_two.at[0], d_two.at[1], d_send.at[1], d_recv.at[1])
    compute(XN)
    first_hop(XN, 0)
    compute(YN)
    first_hop(YN, 1)
    for k in range(2, chunks):
        first_hop(DIAG, k)
    dense_b.wait_recv()
    d_three[0] = d_two[0] + d_two[1]
    dense_c = to(y_next, d_three.at[0], d_three.at[1], d_send.at[2], d_recv.at[2])
    second_hop(XN, 1)
    second_hop(YN, 0)
    compute(OWN)
    dense_c.wait_recv()
    d_four[...] = d_three[0] + d_three[1]
    dense_d = []
    for j in range(1, n_z):
        target = lax.rem(z + j, n_z)
        source = lax.rem(z + n_z - j, n_z)
        copy = pltpu.make_async_remote_copy(
            src_ref=d_four,
            dst_ref=d_z.at[j],
            send_sem=d_send.at[3 + j],
            recv_sem=d_recv.at[3 + j],
            device_id={"expert": target},
            device_id_type=MESH,
        )
        copy.start()
        dense_d.append(copy)
    for k in range(2, chunks):
        first_hop((XN, YN)[k % 2], k)
    for k in range(2, chunks):
        second_hop((YN, XN)[k % 2], k)

    ag = {}
    peers = []
    for i in (5, 6, 7):
        loads[i].wait()

    def at(s, k):
        rows = pl.ds(pl.multiple_of(owners[s] * block, LANES), block)
        return w_out.at[rows, cols(k)]

    def spread(s, k):
        i = s * chunks + k
        peers.append(to(peer, at(s, k), at(s, k), peer_send.at[i], peer_recv.at[i]))

    def finish(k):
        rs[XN, k].wait_recv()
        rs[YN, k].wait_recv()
        gradient = part[OWN, :, cols(k)] + decoded(XN * chunks + k) + decoded(YN * chunks + k)
        master, moment, second = adamw_kernel(
            gradient, p_out[:, cols(k)], m_out[:, cols(k)], v_out[:, cols(k)]
        )
        at(OWN, k)[...] = master.astype(jnp.bfloat16)
        for s, device in ((XN, x_next), (YN, y_next)):
            ag[s, k] = to(
                device,
                at(OWN, k),
                at(OWN, k),
                ag_send.at[s * chunks + k],
                ag_recv.at[s * chunks + k],
            )
        p_out[:, cols(k)] = master
        m_out[:, cols(k)] = moment
        v_out[:, cols(k)] = second
        spread(OWN, k)

    for k in range(chunks):
        finish(k)

    for copy in dense_d:
        copy.wait_recv()
    d_z[0] = d_four[...]
    total = None
    for zz in range(n_z):
        term = d_z[lax.rem(z - zz + n_z, n_z)]
        total = term if total is None else total + term
    d_at = pl.ds(pl.multiple_of(core * half, 8), half)
    d_tot[d_at, :] = total
    dense_e = to(peer, d_tot.at[d_at], d_tot.at[d_at], d_send.at[3], d_recv.at[3])

    for k in range(chunks):
        s, device = ((XN, y_next), (YN, x_next))[k % 2]
        ag[s, k].wait_recv()
        ag[DIAG, k] = to(
            device,
            at(s, k),
            at(s, k),
            ag_send.at[DIAG * chunks + k],
            ag_recv.at[DIAG * chunks + k],
        )
        spread(s, k)
        other = XN + YN - s
        ag[other, k].wait_recv()
        spread(other, k)

    dense_e.wait_recv()
    d_new = adamw_kernel(d_tot[...], dp_ref[...], dm_ref[...], dv_ref[...])
    dp_out[...], dm_out[...], dv_out[...] = d_new

    for k in range(chunks):
        ag[DIAG, k].wait_recv()
        spread(DIAG, k)

    for copy in list(inputs.values()) + [hid_copy, dense_a, dense_b, dense_c, dense_e] + dense_d:
        copy.wait_send()
    for copy in list(rs.values()) + list(ag.values()):
        copy.wait_send()
    for copy in peers:
        copy.wait()


def place_kernel(*refs):
    count = len(refs) // 2
    copies = [
        pltpu.make_async_copy(refs[i], refs[count + i], refs[-1].at[i]) for i in range(count)
    ]
    for copy in copies:
        copy.start()
    for copy in copies:
        copy.wait()


def fused_on_device(
    n_z,
    hidden_act,
    out_grad,
    counts,
    expert_master,
    expert_mom,
    expert_var,
    dense_partial,
    dense_master,
    dense_mom,
    dense_var,
):
    slots, width = hidden_act.shape
    block = expert_master.shape[0]
    chunks = width // LANES
    gains = dense_master.shape[0]
    rows = gains // LANES
    half = rows // 2
    f32, bf16, i16 = jnp.float32, jnp.bfloat16, jnp.int16
    dma = pltpu.SemaphoreType.DMA
    vmem = pl.BlockSpec(memory_space=pltpu.VMEM)
    hbm = pl.BlockSpec(memory_space=pl.ANY)
    outs = pl.pallas_call(
        functools.partial(fused_kernel, n_z),
        out_shape=[
            pltpu.VMEM((out_grad.shape[1], width), bf16),
            *[pltpu.VMEM((block, width), f32)] * 3,
            *[pltpu.VMEM((rows, LANES), f32)] * 3,
        ],
        in_specs=[pl.BlockSpec(memory_space=pltpu.SMEM)] + [hbm] * 5 + [vmem] * 4,
        out_specs=[vmem] * 7,
        scratch_shapes=[
            pltpu.VMEM((slots, width), bf16),
            pltpu.VMEM((slots, width), bf16),
            pltpu.VMEM((slots, width), bf16),
            pltpu.VMEM((4, slots, block), bf16),
            pltpu.VMEM((4, slots, block), bf16),
            pltpu.VMEM((4, block, width), f32),
            pltpu.VMEM((3 * chunks, block + 16, LANES), i16),
            pltpu.VMEM((3 * chunks, block + 16, LANES), i16),
            pltpu.VMEM((half, LANES), f32),
            pltpu.VMEM((2, half, LANES), f32),
            pltpu.VMEM((2, half, LANES), f32),
            pltpu.VMEM((half, LANES), f32),
            pltpu.VMEM((n_z, half, LANES), f32),
            pltpu.VMEM((rows, LANES), f32),
            dma((8,)),
            dma((5,)),
            dma((5,)),
            dma((3 * chunks,)),
            dma((3 * chunks,)),
            dma((3 * chunks,)),
            dma((3 * chunks,)),
            dma((4 * chunks,)),
            dma((4 * chunks,)),
            dma((3 + n_z,)),
            dma((3 + n_z,)),
        ],
        compiler_params=pltpu.CompilerParams(
            collective_id=0, has_side_effects=True, vmem_limit_bytes=44 * 2**20
        ),
    )(
        counts,
        hidden_act,
        out_grad,
        expert_master,
        expert_mom,
        expert_var,
        dense_partial.reshape(rows, LANES),
        dense_master.reshape(rows, LANES),
        dense_mom.reshape(rows, LANES),
        dense_var.reshape(rows, LANES),
    )
    outs = pl.pallas_call(
        place_kernel,
        out_shape=[jax.ShapeDtypeStruct(a.shape, a.dtype) for a in outs],
        in_specs=[hbm] * 7,
        out_specs=[hbm] * 7,
        scratch_shapes=[dma((7,))],
        compiler_params=pltpu.CompilerParams(vmem_limit_bytes=2**20),
    )(*outs)
    return tuple(outs[:4]) + tuple(a.reshape(gains) for a in outs[4:])


def solution(mesh):
    in_specs = (
        P("dp", "expert"),
        P("dp", None),
        P("dp"),
        P("dp", "expert"),
        P("dp", "expert"),
        P("dp", "expert"),
        P("dp", "expert", None),
        P(),
        P(),
        P(),
    )
    out_specs = (
        P(None, "expert"),
        P("dp", "expert"),
        P("dp", "expert"),
        P("dp", "expert"),
        P(),
        P(),
        P(),
    )
    body = on_device
    if mesh.shape["dp"] == 8:
        body = functools.partial(fused_on_device, mesh.shape["expert"])
    return jax.shard_map(
        body, mesh=mesh, in_specs=in_specs, out_specs=out_specs, check_vma=False
    )
```

```python
import functools

import jax
import jax.numpy as jnp
from jax import lax
from jax.experimental import pallas as pl
from jax.experimental.pallas import tpu as pltpu
from jax.sharding import PartitionSpec as P

beta_one = 0.9
beta_two = 0.95
learn_rate = 0.00022
decay_rate = 0.1
epsilon = 1e-08
step_count = 100


def adamw(gradient, master, moment, second):
    moment_new = beta_one * moment + (1.0 - beta_one) * gradient
    second_new = beta_two * second + (1.0 - beta_two) * gradient * gradient
    first_fix = 1.0 - beta_one**step_count
    second_fix = 1.0 - beta_two**step_count
    update = (
        moment_new / first_fix / (jnp.sqrt(second_new / second_fix) + epsilon) + decay_rate * master
    )
    return (master - learn_rate * update, moment_new, second_new)


def on_device(
    hidden_act,
    out_grad,
    counts,
    expert_master,
    expert_mom,
    expert_var,
    dense_partial,
    dense_master,
    dense_mom,
    dense_var,
):
    slots = hidden_act.shape[0]
    row_live = lax.iota(jnp.int32, slots) < counts[0]
    masked = jnp.where(row_live[:, None], hidden_act, jnp.zeros_like(hidden_act))
    dense_local = dense_partial.reshape(-1)
    expert_grad = lax.psum_scatter(
        lax.dot_general(
            out_grad, masked, (((0,), (0,)), ((), ())), preferred_element_type=jnp.float32
        ),
        "dp",
        scatter_dimension=0,
        tiled=True,
    )
    dense_grad = lax.psum(dense_local, ("dp", "expert"))
    dense_new, dense_moment, dense_second = adamw(dense_grad, dense_master, dense_mom, dense_var)
    master_new, moment_new, second_new = adamw(expert_grad, expert_master, expert_mom, expert_var)
    routed_weight = lax.all_gather(master_new.astype(jnp.bfloat16), "dp", axis=0, tiled=True)
    return (
        routed_weight,
        master_new,
        moment_new,
        second_new,
        dense_new,
        dense_moment,
        dense_second,
    )


MESH = pl.DeviceIdType.MESH
LANES = 128
DIAG, XN, YN, OWN = 0, 1, 2, 3
TOP = 32767.0


def adamw_kernel(gradient, master, moment, second):
    moment_new = beta_one * moment + (1.0 - beta_one) * gradient
    second_new = beta_two * second + (1.0 - beta_two) * gradient * gradient
    first_fix = 1.0 / (1.0 - beta_one**step_count)
    second_fix = 1.0 / (1.0 - beta_two**step_count)
    update = (
        moment_new * first_fix / (jnp.sqrt(second_new * second_fix) + epsilon) + decay_rate * master
    )
    return (master - learn_rate * update, moment_new, second_new)


def fused_kernel(
    n_z,
    counts_ref,
    hid_ref,
    og_ref,
    p_ref,
    m_ref,
    v_ref,
    dpart_hbm,
    dp_hbm,
    dm_hbm,
    dv_hbm,
    w_out,
    p_out,
    m_out,
    v_out,
    dp_out,
    dm_out,
    dv_out,
    dpart_ref,
    dp_ref,
    dm_ref,
    dv_ref,
    hid_raw,
    hid_own,
    hid_peer,
    og_own,
    og_peer,
    part,
    q_send,
    q_recv,
    d_one,
    d_two,
    d_three,
    d_four,
    d_z,
    d_tot,
    load_sem,
    in_send,
    in_recv,
    rs_send,
    rs_recv,
    ag_send,
    ag_recv,
    peer_send,
    peer_recv,
    d_send,
    d_recv,
):
    me = lax.axis_index("dp")
    z = lax.axis_index("expert")
    core = lax.rem(me, 2)
    x_at = lax.rem(lax.div(me, 2), 2)
    y_at = lax.div(me, 4)
    flip = 1 - 2 * core
    peer = me + flip
    x_next = me + 2 - 4 * x_at
    y_next = me + 4 - 8 * y_at
    diag = x_next + 4 - 8 * y_at
    owners = (diag, x_next, y_next, me)
    block = p_ref.shape[0]
    width = p_ref.shape[1]
    chunks = width // LANES
    half = d_one.shape[0]

    def og_cols(device):
        return og_ref.at[:, pl.ds(pl.multiple_of(device * block, LANES), block)]

    def cols(k):
        return pl.ds(k * LANES, LANES)

    loads = [pltpu.make_async_copy(hid_ref, hid_raw, load_sem.at[0])]
    for s in range(4):
        loads.append(pltpu.make_async_copy(og_cols(owners[s]), og_own.at[s], load_sem.at[1 + s]))
    for i, (a, b) in enumerate(((p_ref, p_out), (m_ref, m_out), (v_ref, v_out))):
        loads.append(pltpu.make_async_copy(a, b, load_sem.at[5 + i]))
    gain_pairs = ((dpart_hbm, dpart_ref), (dp_hbm, dp_ref), (dm_hbm, dm_ref), (dv_hbm, dv_ref))
    for i, (a, b) in enumerate(gain_pairs):
        loads.append(pltpu.make_async_copy(a, b, load_sem.at[8 + i]))
    for copy in loads:
        copy.start()

    barrier = pltpu.get_barrier_semaphore()
    for device in (peer, x_next, y_next):
        pl.semaphore_signal(barrier, inc=1, device_id={"dp": device}, device_id_type=MESH)
    for j in range(1, n_z):
        pl.semaphore_signal(
            barrier, inc=1, device_id={"expert": lax.rem(z + j, n_z)}, device_id_type=MESH
        )
    pl.semaphore_wait(barrier, 3 + n_z - 1)

    def to(device, src, dst, send, recv):
        copy = pltpu.make_async_remote_copy(
            src_ref=src,
            dst_ref=dst,
            send_sem=send,
            recv_sem=recv,
            device_id={"dp": device},
            device_id_type=MESH,
        )
        copy.start()
        return copy

    sends = []
    inputs = {}

    def send_input(s):
        inputs[s] = to(
            peer, og_cols(owners[s] + flip), og_peer.at[s], in_send.at[s], in_recv.at[s]
        )

    send_input(DIAG)
    loads[0].wait()
    live = lax.broadcasted_iota(jnp.int32, hid_raw.shape, 0) < counts_ref[0]
    hid_own[...] = jnp.where(live, hid_raw[...].astype(jnp.float32), 0.0).astype(jnp.bfloat16)
    hid_copy = to(peer, hid_own, hid_peer, in_send.at[4], in_recv.at[4])
    loads[8].wait()
    dense_a = to(
        peer,
        dpart_ref.at[pl.ds(pl.multiple_of((1 - core) * half, 8), half)],
        d_one,
        d_send.at[0],
        d_recv.at[0],
    )
    for s in (XN, YN, OWN):
        send_input(s)

    def compute(s, lo=0, hi=None):
        hi = width if hi is None else hi
        if lo == 0:
            loads[1 + s].wait()
            if s == DIAG:
                hid_copy.wait_recv()
            inputs[s].wait_recv()

        @pl.loop(0, block // LANES)
        def _(t):
            at = pl.ds(pl.multiple_of(t * LANES, LANES), LANES)
            dims = (((0,), (0,)), ((), ()))
            part[s, at, lo:hi] = lax.dot_general(
                og_own[s, :, at], hid_own[:, lo:hi], dims, preferred_element_type=jnp.float32
            ) + lax.dot_general(
                og_peer[s, :, at], hid_peer[:, lo:hi], dims, preferred_element_type=jnp.float32
            )

    def decoded(i):
        scale = jnp.exp2(q_recv[i, pl.ds(block, 16), :].astype(jnp.int32)[0:1].astype(jnp.float32) * (1.0 / 256.0))
        return q_recv[i, pl.ds(0, block), :].astype(jnp.int32).astype(jnp.float32) * scale

    rs = {}

    def send_sum(device, s, k, value=None):
        i = s * chunks + k
        if value is None:
            value = part[s, :, cols(k)]
        top = jnp.max(jnp.abs(value), axis=0, keepdims=True)
        level = jnp.ceil(jnp.log2(jnp.maximum(top, 1e-30) * (1.0 / TOP)) * 256.0) + 1.0
        q = jnp.round(value * jnp.exp2(level * (-1.0 / 256.0)))
        q_send[i, pl.ds(0, block), :] = q.astype(jnp.int32).astype(jnp.int16)
        q_send[i, pl.ds(block, 16), :] = (
            jnp.broadcast_to(level, (16, LANES)).astype(jnp.int32).astype(jnp.int16)
        )
        rs[s, k] = to(device, q_send.at[i], q_recv.at[i], rs_send.at[i], rs_recv.at[i])

    def first_hop(s, k):
        send_sum((x_next, y_next)[k % 2] if s == DIAG else owners[s], s, k)

    def second_hop(s, k):
        rs[DIAG, k].wait_recv()
        send_sum(owners[s], s, k, part[s, :, cols(k)] + decoded(DIAG * chunks + k))

    split = width // 2
    compute(DIAG, 0, split)
    first_hop(DIAG, 0)
    first_hop(DIAG, 1)
    dense_a.wait_recv()
    d_two[0] = dpart_ref[pl.ds(pl.multiple_of(core * half, 8), half), :] + d_one[...]
    dense_b = to(x_next, d_two.at[0], d_two.at[1], d_send.at[1], d_recv.at[1])
    compute(XN)
    first_hop(XN, 0)
    compute(YN)
    first_hop(YN, 1)
    compute(DIAG, split)
    for k in range(2, chunks):
        first_hop(DIAG, k)
    dense_b.wait_recv()
    d_three[0] = d_two[0] + d_two[1]
    dense_c = to(y_next, d_three.at[0], d_three.at[1], d_send.at[2], d_recv.at[2])
    second_hop(XN, 1)
    second_hop(YN, 0)
    compute(OWN)
    dense_c.wait_recv()
    d_four[...] = d_three[0] + d_three[1]
    dense_d = []
    for j in range(1, n_z):
        target = lax.rem(z + j, n_z)
        source = lax.rem(z + n_z - j, n_z)
        copy = pltpu.make_async_remote_copy(
            src_ref=d_four,
            dst_ref=d_z.at[j],
            send_sem=d_send.at[3 + j],
            recv_sem=d_recv.at[3 + j],
            device_id={"expert": target},
            device_id_type=MESH,
        )
        copy.start()
        dense_d.append(copy)
    for k in range(2, chunks):
        first_hop((XN, YN)[k % 2], k)
    for k in range(2, chunks):
        second_hop((YN, XN)[k % 2], k)

    ag = {}
    peers = []
    for i in (5, 6, 7):
        loads[i].wait()

    def at(s, k):
        rows = pl.ds(pl.multiple_of(owners[s] * block, LANES), block)
        return w_out.at[rows, cols(k)]

    def spread(s, k):
        i = s * chunks + k
        peers.append(to(peer, at(s, k), at(s, k), peer_send.at[i], peer_recv.at[i]))

    def finish(k):
        rs[XN, k].wait_recv()
        rs[YN, k].wait_recv()
        gradient = part[OWN, :, cols(k)] + decoded(XN * chunks + k) + decoded(YN * chunks + k)
        master, moment, second = adamw_kernel(
            gradient, p_out[:, cols(k)], m_out[:, cols(k)], v_out[:, cols(k)]
        )
        at(OWN, k)[...] = master.astype(jnp.bfloat16)
        for s, device in ((XN, x_next), (YN, y_next)):
            ag[s, k] = to(
                device,
                at(OWN, k),
                at(OWN, k),
                ag_send.at[s * chunks + k],
                ag_recv.at[s * chunks + k],
            )
        p_out[:, cols(k)] = master
        m_out[:, cols(k)] = moment
        v_out[:, cols(k)] = second
        spread(OWN, k)

    for k in range(chunks):
        finish(k)

    for copy in dense_d:
        copy.wait_recv()
    d_z[0] = d_four[...]
    total = None
    for zz in range(n_z):
        term = d_z[lax.rem(z - zz + n_z, n_z)]
        total = term if total is None else total + term
    d_at = pl.ds(pl.multiple_of(core * half, 8), half)
    d_tot[d_at, :] = total
    dense_e = to(peer, d_tot.at[d_at], d_tot.at[d_at], d_send.at[3], d_recv.at[3])

    for k in range(chunks):
        s, device = ((XN, y_next), (YN, x_next))[k % 2]
        ag[s, k].wait_recv()
        ag[DIAG, k] = to(
            device,
            at(s, k),
            at(s, k),
            ag_send.at[DIAG * chunks + k],
            ag_recv.at[DIAG * chunks + k],
        )
        spread(s, k)
        other = XN + YN - s
        ag[other, k].wait_recv()
        spread(other, k)

    dense_e.wait_recv()
    for i in (9, 10, 11):
        loads[i].wait()
    d_new = adamw_kernel(d_tot[...], dp_ref[...], dm_ref[...], dv_ref[...])
    dp_out[...], dm_out[...], dv_out[...] = d_new

    for k in range(chunks):
        ag[DIAG, k].wait_recv()
        spread(DIAG, k)

    for copy in list(inputs.values()) + [hid_copy, dense_a, dense_b, dense_c, dense_e] + dense_d:
        copy.wait_send()
    for copy in list(rs.values()) + list(ag.values()):
        copy.wait_send()
    for copy in peers:
        copy.wait()


def place_kernel(*refs):
    count = len(refs) // 2
    copies = [
        pltpu.make_async_copy(refs[i], refs[count + i], refs[-1].at[i]) for i in range(count)
    ]
    for copy in copies:
        copy.start()
    for copy in copies:
        copy.wait()


def fused_on_device(
    n_z,
    hidden_act,
    out_grad,
    counts,
    expert_master,
    expert_mom,
    expert_var,
    dense_partial,
    dense_master,
    dense_mom,
    dense_var,
):
    slots, width = hidden_act.shape
    block = expert_master.shape[0]
    chunks = width // LANES
    gains = dense_master.shape[0]
    rows = gains // LANES
    half = rows // 2
    f32, bf16, i16 = jnp.float32, jnp.bfloat16, jnp.int16
    dma = pltpu.SemaphoreType.DMA
    vmem = pl.BlockSpec(memory_space=pltpu.VMEM)
    hbm = pl.BlockSpec(memory_space=pl.ANY)
    outs = pl.pallas_call(
        functools.partial(fused_kernel, n_z),
        out_shape=[
            pltpu.VMEM((out_grad.shape[1], width), bf16),
            *[pltpu.VMEM((block, width), f32)] * 3,
            *[pltpu.VMEM((rows, LANES), f32)] * 3,
        ],
        in_specs=[pl.BlockSpec(memory_space=pltpu.SMEM)] + [hbm] * 9,
        out_specs=[vmem] * 7,
        scratch_shapes=[
            *[pltpu.VMEM((rows, LANES), f32)] * 4,
            pltpu.VMEM((slots, width), bf16),
            pltpu.VMEM((slots, width), bf16),
            pltpu.VMEM((slots, width), bf16),
            pltpu.VMEM((4, slots, block), bf16),
            pltpu.VMEM((4, slots, block), bf16),
            pltpu.VMEM((4, block, width), f32),
            pltpu.VMEM((3 * chunks, block + 16, LANES), i16),
            pltpu.VMEM((3 * chunks, block + 16, LANES), i16),
            pltpu.VMEM((half, LANES), f32),
            pltpu.VMEM((2, half, LANES), f32),
            pltpu.VMEM((2, half, LANES), f32),
            pltpu.VMEM((half, LANES), f32),
            pltpu.VMEM((n_z, half, LANES), f32),
            pltpu.VMEM((rows, LANES), f32),
            dma((12,)),
            dma((5,)),
            dma((5,)),
            dma((3 * chunks,)),
            dma((3 * chunks,)),
            dma((3 * chunks,)),
            dma((3 * chunks,)),
            dma((4 * chunks,)),
            dma((4 * chunks,)),
            dma((3 + n_z,)),
            dma((3 + n_z,)),
        ],
        compiler_params=pltpu.CompilerParams(
            collective_id=0, has_side_effects=True, vmem_limit_bytes=44 * 2**20
        ),
    )(
        counts,
        hidden_act,
        out_grad,
        expert_master,
        expert_mom,
        expert_var,
        dense_partial.reshape(rows, LANES),
        dense_master.reshape(rows, LANES),
        dense_mom.reshape(rows, LANES),
        dense_var.reshape(rows, LANES),
    )
    outs = pl.pallas_call(
        place_kernel,
        out_shape=[jax.ShapeDtypeStruct(a.shape, a.dtype) for a in outs],
        in_specs=[hbm] * 7,
        out_specs=[hbm] * 7,
        scratch_shapes=[dma((7,))],
        compiler_params=pltpu.CompilerParams(vmem_limit_bytes=2**20),
    )(*outs)
    return tuple(outs[:4]) + tuple(a.reshape(gains) for a in outs[4:])


def solution(mesh):
    in_specs = (
        P("dp", "expert"),
        P("dp", None),
        P("dp"),
        P("dp", "expert"),
        P("dp", "expert"),
        P("dp", "expert"),
        P("dp", "expert", None),
        P(),
        P(),
        P(),
    )
    out_specs = (
        P(None, "expert"),
        P("dp", "expert"),
        P("dp", "expert"),
        P("dp", "expert"),
        P(),
        P(),
        P(),
    )
    body = on_device
    if mesh.shape["dp"] == 8:
        body = functools.partial(fused_on_device, mesh.shape["expert"])
    return jax.shard_map(
        body, mesh=mesh, in_specs=in_specs, out_specs=out_specs, check_vma=False
    )
```
